256 devices in a mesh: row: 32 (over y, z_hi, core), col: 8 (over x, z_lo).
Axes of the slice: x: 4, y: 4, z: 8 (z_hi: 4, z_lo: 2; z = z_hi * 2 + z_lo), core: 2. Of those that a mesh axis runs over, the one named last changes fastest.
Arguments:
- vectors: float32 [8192, 32768], P(('row', 'col')), may hold values from -6 to 6
- reflectors: float32 [6, 128, 32768], P(None, 'col', 'row')
- factors: float32 [6, 128, 128], replicated, as said below
Outputs:
- transformed: float32 [8192, 32768], P('col', 'row')
The draws below stay inside these ranges and needn't reach their ends.
Inputs may be any that keep to these rules, and one draw needn't show every extreme that they name: factors[k] is upper triangular, and its inverse equals the strict upper part of reflectors[k] reflectors[k]^T plus half of that product's diagonal, so each panel is orthogonal.
All inputs are finite; a program needn't handle non-finite values.
Results may differ from the reference program's by a relative error of at most 0.0001.
Values sent between devices are 32-bit elements; how exact they have to be, the bound alone decides.
A program may use at most 128 MiB of HBM per device.

```python
import jax
import jax.numpy as jnp
from jax import lax

N = 32768
BLOCK = 128
PANELS = 6
EIGVECS = 8192


def invert_upper(matrix):
    identity = jnp.eye(matrix.shape[0], dtype=jnp.float32)
    return jax.scipy.linalg.solve_triangular(matrix, identity, lower=False)


def reflector_pair(key):
    random_part = jax.random.normal(jax.random.fold_in(key, 11), (PANELS, BLOCK, N), jnp.float32) / jnp.sqrt(jnp.float32(N))
    mixing = jnp.eye(BLOCK, dtype=jnp.float32) + 0.35 / jnp.sqrt(jnp.float32(BLOCK)) * jax.random.normal(jax.random.fold_in(key, 12), (PANELS, BLOCK, BLOCK), jnp.float32)
    reflect = jnp.einsum('pij,pjn->pin', mixing, random_part, precision=lax.Precision.HIGHEST)
    gram_matrix = jnp.einsum('pin,pjn->pij', reflect, reflect, precision=lax.Precision.HIGHEST)
    diagonal_half = 0.5 * jnp.einsum('pii->pi', gram_matrix)
    inverse = jnp.triu(gram_matrix, 1) + jax.vmap(jnp.diag)(diagonal_half)
    triangle = jax.vmap(invert_upper)(inverse)
    return (reflect, triangle)


def draw_reflectors(key, part):
    return reflector_pair(jax.random.fold_in(key, 7))[0]


def draw_factors(key, part):
    return reflector_pair(jax.random.fold_in(key, 7))[1]


def levels(own_key, extent, cuts, low, largest):
    gain = 1.0
    for position, shards_of in cuts:
        steps = jax.random.uniform(jax.random.fold_in(jax.random.fold_in(own_key, 6), position), (shards_of,), jnp.float32, low / len(cuts), largest / len(cuts))
        gain = gain * jnp.repeat(jnp.exp(steps), extent[position] // shards_of).reshape((-1,) + (1,) * (len(extent) - 1 - position))
    return gain


def gaussian(rng, extent, width, limit, pieces=(), kind=jnp.bfloat16):
    result = jax.random.normal(rng, extent, jnp.float32) * width
    if len(pieces) > 0:
        result = levels(rng, extent, pieces, -0.22, 0.18) * result
    return jnp.clip(result, min=-limit, max=limit).astype(kind)


def setup_inputs(seed: int = 0) -> dict:
    keys = jax.random.split(jax.random.key(seed), 4)
    return {
        "vectors": gaussian(keys[0], (EIGVECS, N), 1.0, 6.0, ((0, 256),), jnp.float32),
        "reflectors": draw_reflectors(jax.random.fold_in(keys[3], 71), 0),
        "factors": draw_factors(jax.random.fold_in(keys[3], 71), 0),
    }


def reference(vectors, reflectors, factors):
    current = vectors
    for panel in range(PANELS - 1, -1, -1):
        stacked = reflectors[panel]
        projection = lax.dot_general(current.astype(jnp.float32), stacked.astype(jnp.float32), (((1,), (1,)), ((), ())), precision=lax.Precision.HIGHEST, preferred_element_type=jnp.float32)
        update = jnp.dot(projection.astype(jnp.float32), factors[panel].T.astype(jnp.float32), precision=lax.Precision.HIGHEST, preferred_element_type=jnp.float32)
        current = current - jnp.dot(update.astype(jnp.float32), stacked.astype(jnp.float32), precision=lax.Precision.HIGHEST, preferred_element_type=jnp.float32)
    return current
```

```python
import jax
import jax.numpy as jnp
from jax import lax
from jax.experimental import pallas as pl
from jax.experimental.pallas import tpu as pltpu
from jax.sharding import Mesh
from jax.sharding import PartitionSpec as P

ROW = ("row_0", "row_1", "row_2")
ROW_COL = ("row_0", "row_1", "row_2", "col")


def split_up(value, dim, length):
    dims = value.shape
    parts = value.reshape(*dims[:dim], length, dims[dim] // length, *dims[dim + 1 :])
    return jnp.moveaxis(parts, dim, 0)


def sum_at_owner(value, axis, dim):
    parts = split_up(value, dim, lax.axis_size(axis))
    arrived = lax.all_to_all(parts, axis, split_axis=0, concat_axis=0, tiled=True)
    return arrived.sum(axis=0)


def summed_rows(value, axes, dim):
    far, near = axes
    parts = split_up(value, dim, lax.axis_size(far))
    nearer = sum_at_owner(parts, near, dim + 1)
    arrived = lax.all_to_all(nearer, far, split_axis=0, concat_axis=0, tiled=True)
    return arrived.sum(axis=0)


def padded_to(lines, length):
    spare = -len(lines) % length
    return jnp.pad(lines, [(0, spare)] + [(0, 0)] * (lines.ndim - 1))


def sent_to_all(value, axis):
    copies = jnp.broadcast_to(value, (lax.axis_size(axis), *value.shape))
    return lax.all_to_all(copies, axis, split_axis=0, concat_axis=0, tiled=True)


def laid_out(parts, dim):
    parts = jnp.moveaxis(parts, 0, dim)
    dims = parts.shape
    return parts.reshape(*dims[:dim], dims[dim] * dims[dim + 1], *dims[dim + 2 :])


def whole_of(value, axes, dim):
    far, near = axes
    first = sent_to_all(value, far)
    parts = jnp.swapaxes(sent_to_all(first, near), 0, 1)
    return laid_out(parts.reshape(-1, *value.shape), dim)


def sum_by_parts(value, axes):
    own = summed_rows(padded_to(value, lax.axis_size(axes[0]) * lax.axis_size(axes[1])), axes, 0)
    whole = whole_of(own, axes, 0)
    return whole[: len(value)].reshape(value.shape)


def in_one(arrays, axis):
    ends = [0]
    for a in arrays:
        ends.append(ends[-1] + a.size)
    subtotal = sum_by_parts(jnp.concatenate([a.ravel() for a in arrays]), axis)
    return tuple((subtotal[b:e].reshape(a.shape) for a, b, e in zip(arrays, ends, ends[1:])))


def product(left, right):
    return jnp.dot(left, right, precision=lax.Precision.HIGHEST, preferred_element_type=jnp.float32)


def against(left, right):
    return lax.dot_general(
        left,
        right,
        (((1,), (1,)), ((), ())),
        precision=lax.Precision.HIGHEST,
        preferred_element_type=jnp.float32,
    )


def place(row_far, row_near, col):
    return (row_far, row_near // 2, row_near % 2, col)


def exchange_kernel(vec, out, held, sent_a, came_a, sent_b, came_b, local):
    y, near = lax.axis_index("row_0"), lax.axis_index("row_1") * 2 + lax.axis_index("row_2")
    col = lax.axis_index("col")
    slot = (near % 4) * 8 + col
    rows = vec.shape[0]
    piece = vec.shape[1] // 32
    mesh_id = pl.DeviceIdType.MESH
    barrier = pltpu.get_barrier_semaphore()
    for k in range(1, 4):
        pl.semaphore_signal(barrier, inc=1, device_id=place((y + k) % 4, near, col), device_id_type=mesh_id)
    for k in range(4):
        for w in range(8):
            pl.semaphore_signal(barrier, inc=1, device_id=place(y, w, k * 2 + near // 4), device_id_type=mesh_id)
    for w in range(4):
        for c in range(8):
            pl.semaphore_signal(barrier, inc=1, device_id=place(y, (col % 2) * 4 + w, c), device_id_type=mesh_id)
    pl.semaphore_wait(barrier, 3 + 64)

    def columns(far, w):
        return vec.at[:, pl.ds(pl.multiple_of((far * 8 + w) * piece, piece), piece)]

    def first(k, w):
        far = (y + k) % 4
        return pltpu.make_async_remote_copy(
            src_ref=columns(far, w), dst_ref=held.at[k - 1, w],
            send_sem=sent_a.at[k - 1, w], recv_sem=came_a.at[k - 1, w],
            device_id=place(far, near, col), device_id_type=mesh_id,
        )

    def second(k, w, start):
        origin = (y - k) % 4
        source = held.at[k - 1, w] if k else columns(y, w)
        target = out.at[pl.ds(pl.multiple_of(slot * rows, rows), rows), :]
        there = origin * 2 + near // 4
        mine = jnp.logical_and(w == near, there == col)

        @pl.when(mine)
        def _():
            copy = pltpu.make_async_copy(source, target, local)
            copy.start() if start else copy.wait()

        @pl.when(jnp.logical_not(mine))
        def _():
            copy = pltpu.make_async_remote_copy(
                src_ref=source, dst_ref=target, send_sem=sent_b.at[k, w], recv_sem=came_b.at[slot],
                device_id=place(y, w, there), device_id_type=mesh_id,
            )
            copy.start() if start else copy.wait_send()

    for i in range(8):
        for k in (1, 3, 2):
            first(k, near ^ i).start()
    for i in range(8):
        second(0, near ^ i, True)
    for i in range(8):
        for k in (1, 3, 2):
            first(k, near ^ i).wait_recv()
            second(k, near ^ i, True)
    for s in range(32):
        relayed_here = jnp.logical_and(near == (col % 2) * 4 + s // 8, col == s % 8)

        @pl.when(jnp.logical_not(relayed_here))
        def _():
            block = out.at[pl.ds(s * rows, rows), :]
            pltpu.make_async_remote_copy(
                src_ref=block, dst_ref=block, send_sem=sent_b.at[0, 0], recv_sem=came_b.at[s],
                device_id=place(y, near, col), device_id_type=mesh_id,
            ).wait_recv()
    for k in range(4):
        for w in range(8):
            second(k, w, False)
            if k:
                first(k, w).wait_send()


def exchanged(vectors):
    rows, length = vectors.shape
    piece = length // 32
    return pl.pallas_call(
        exchange_kernel,
        out_shape=jax.ShapeDtypeStruct((rows * 32, piece), jnp.float32),
        in_specs=[pl.BlockSpec(memory_space=pl.ANY)],
        out_specs=pl.BlockSpec(memory_space=pl.ANY),
        scratch_shapes=[
            pltpu.VMEM((3, 8, rows, piece), jnp.float32),
            pltpu.SemaphoreType.DMA((3, 8)),
            pltpu.SemaphoreType.DMA((3, 8)),
            pltpu.SemaphoreType.DMA((4, 8)),
            pltpu.SemaphoreType.DMA((32,)),
            pltpu.SemaphoreType.DMA,
        ],
        compiler_params=pltpu.CompilerParams(collective_id=1, has_side_effects=True),
        cost_estimate=pl.CostEstimate(flops=10**9, bytes_accessed=2**23, transcendentals=0),
    )(vectors)


def on_device(vectors, reflectors, factors):
    piece_length = vectors.shape[1] // lax.axis_size(ROW)
    current = exchanged(vectors)
    panels = lax.all_gather(reflectors, "col", axis=1, tiled=True)
    count = panels.shape[0]
    width = panels.shape[1]
    stacked_all = panels.reshape(count * width, piece_length)
    partial_value = against(current, stacked_all)
    pair_list = []
    for first in range(count):
        for second in range(first + 1, count):
            pair_list.append(against(panels[first], panels[second]))
    crossed = jnp.stack(pair_list, axis=0)
    projection, crossed = in_one((partial_value, crossed), (("row_0", "row_1"), "row_2"))
    lookup = {}
    position = 0
    for first in range(count):
        for second in range(first + 1, count):
            lookup[first, second] = crossed[position]
            position = position + 1
    blocks_of = {}
    for second in range(count):
        blocks_of[second, second] = factors[second]
        for first in range(second - 1, -1, -1):
            total = jnp.zeros((width, width), jnp.float32)
            for middle in range(first + 1, second + 1):
                total = total + product(lookup[first, middle], blocks_of[middle, second])
            blocks_of[first, second] = -product(factors[first], total)
    block_rows = []
    for first in range(count):
        pieces = []
        for second in range(count):
            if second < first:
                pieces.append(jnp.zeros((width, width), jnp.float32))
            else:
                pieces.append(blocks_of[first, second])
        block_rows.append(jnp.concatenate(pieces, axis=1))
    factor_all = jnp.concatenate(block_rows, axis=0)
    update = against(projection, factor_all)
    current = current - product(update, stacked_all)
    return current


def solution(mesh):
    finer = Mesh(
        mesh.devices.reshape(4, 4, 2, mesh.shape["col"]), ("row_0", "row_1", "row_2", "col")
    )
    placed = (P(ROW_COL, None), P(None, "col", ROW), P())
    return jax.shard_map(
        on_device, mesh=finer, in_specs=placed, out_specs=P("col", ROW), check_vma=False
    )
```

```python
import jax
import jax.numpy as jnp
from jax import lax
from jax.experimental import pallas as pl
from jax.experimental.pallas import tpu as pltpu
from jax.sharding import PartitionSpec as P

F32 = jnp.float32
BF16 = jnp.bfloat16
MESH = pl.DeviceIdType.MESH
CHUNKS = 4
NT = (((1,), (1,)), ((), ()))
NN = (((1,), (0,)), ((), ()))


def halves(value):
    high = value.astype(BF16)
    return high, (value - high.astype(F32)).astype(BF16)


def dot3(left, right, dims):
    def one(a, b):
        return lax.dot_general(a, b, dims, preferred_element_type=F32)

    return one(left[0], right[0]) + (one(left[0], right[1]) + one(left[1], right[0]))


def part(index, size):
    return pl.ds(pl.multiple_of(index * size, size), size)


def kernel(
    vec, refl, factors, out,
    x, held, panels, vh, vl, xh, xl, uh, ul, proj, r1, r2, s2, r3, upd,
    gp, g1, gs, g2, gc, gall, th, tl,
    sent_a, came_a, sent_b, came_b, sent_v, came_v, own_v, sent_g, came_g, sent_p, came_p,
):
    row, col = lax.axis_index("row"), lax.axis_index("col")
    y, near = row // 8, row % 8
    zh, core = near // 2, near % 2
    far_x, zl = col // 2, col % 2
    slot = (near % 4) * 8 + col
    upper = near // 4
    count, block, piece = panels.shape
    own = refl.shape[1]
    pending = []

    def at(y_, zh_, core_, col_):
        return (y_ * 8 + zh_ * 2 + core_, col_)

    def in_y(k):
        return at((y + k) % 4, zh, core, col)

    def in_z(k):
        return at(y, (zh + k) % 4, core, col)

    def in_x(k):
        return (row, ((far_x + k) % 4) * 2 + zl)

    twin = at(y, zh, 1 - core, col)

    def remote(src, dst, send_sem, recv_sem, device):
        return pltpu.make_async_remote_copy(
            src_ref=src, dst_ref=dst, send_sem=send_sem, recv_sem=recv_sem,
            device_id=device, device_id_type=MESH,
        )

    def send(*args):
        copy = remote(*args)
        copy.start()
        pending.append(copy)
        return copy

    barrier = pltpu.get_barrier_semaphore()
    greeted = []
    for k in range(4):
        for w in range(8):
            greeted.append((y * 8 + w, k * 2 + upper))
    for w in range(4):
        for c in range(8):
            greeted.append((y * 8 + zl * 4 + w, c))
    for o in range(1, 8):
        greeted.append(at((y + o // 2) % 4, zh, (core + o) % 2, col))
        greeted.append((row, (col + o) % 8))
    for k in range(1, 4):
        greeted.append(in_z(k))
    for device in greeted:
        pl.semaphore_signal(barrier, inc=1, device_id=device, device_id_type=MESH)
    pl.semaphore_wait(barrier, len(greeted))

    mine = panels.at[:, part(col, own), :]
    others = panels.at[:, part(far_x * 2 + 1 - zl, own), :]
    keep = pltpu.make_async_copy(refl, mine, own_v)
    keep.start()
    beside = send(refl, mine, sent_v.at[0], came_v.at[0], (row, far_x * 2 + 1 - zl))
    from_x = [send(refl, mine, sent_v.at[k], came_v.at[k], in_x(k)) for k in (1, 3, 2)]

    first = {}
    for c in range(CHUNKS):
        for k in (1, 3, 2):
            first[c, k] = send(
                vec.at[pl.ds(c * 8, 8), part((y + k) % 4, 8 * piece)], held.at[c, k - 1],
                sent_a.at[c, k - 1], came_a.at[c, k - 1], in_y(k),
            )

    local = zl == upper

    def second(c):
        for k in (0, 1, 3, 2):
            if k:
                first[c, k].wait_recv()
            there = ((y - k) % 4) * 2 + upper
            for flip in range(2):
                for j in (1, 3, 2, 0):
                    to_zh, to_core = (zh + j) % 4, (core + flip) % 2
                    w = to_zh * 2 + to_core
                    if k:
                        source = held.at[c, k - 1, :, part(w, piece)]
                    else:
                        source = vec.at[pl.ds(c * 8, 8), part(y * 8 + w, piece)]
                    target = x.at[c, part(slot, 8), :]
                    copy = remote(source, target, sent_b.at[c], came_b.at[c], at(y, to_zh, to_core, there))
                    if flip or j:
                        copy.start()
                    else:

                        @pl.when(there == col)
                        def _(source=source, target=target):
                            pltpu.make_async_copy(source, target, came_b.at[c]).start()

                        @pl.when(there != col)
                        def _(copy=copy):
                            copy.start()

    second(0)
    beside.wait_recv()
    from_z = [send(others, others, sent_v.at[3 + k], came_v.at[3 + k], in_x(k)) for k in (1, 3, 2)]
    for copy in from_x + from_z:
        copy.wait_recv()
    keep.wait()
    for k in range(count):
        vh[k], vl[k] = halves(panels[k])

    line = col % count
    for d in range(1, 4):
        other = (line + d) % count
        low, high = jnp.minimum(line, other), jnp.maximum(line, other)
        gp[d - 1] = dot3((vh[low], vl[low]), (vh[high], vl[high]), NT)
    lot = block // 8
    step_1 = []
    for o in range(1, 8):
        to_y, to_core = (y + o // 2) % 4, (core + o) % 2
        step_1.append(
            send(
                gp.at[:, part(to_core * 4 + to_y, lot), :], g1.at[o - 1],
                sent_g.at[0, o], came_g.at[0, o], at(to_y, zh, to_core, col),
            )
        )
    second(1)
    for copy in step_1:
        copy.wait_recv()
    total = gp[:, part(core * 4 + y, lot), :]
    for o in range(7):
        total = total + g1[o]
    gs[...] = total
    step_2 = [send(gs, g2.at[k - 1], sent_g.at[1, k], came_g.at[1, k], in_z(k)) for k in (1, 3, 2)]

    def g_col():
        for copy in step_2:
            copy.wait_recv()
        gc[col] = gs[...] + g2[0] + (g2[1] + g2[2])
        return [
            send(gc.at[col], gc.at[col], sent_g.at[2, k], came_g.at[2, k], (row, (col + k) % 8))
            for k in range(1, 8)
        ]

    def g_y(before):
        for copy in before:
            copy.wait_recv()
        lines = part(core * 4 + y, lot)
        gall[:, :, lines, :] = gc[pl.ds(0, count)]
        return [
            send(
                gc.at[pl.ds(0, count)], gall.at[:, :, lines, :],
                sent_g.at[3, k], came_g.at[3, k], in_y(k),
            )
            for k in (1, 3, 2)
        ]

    def g_core(before):
        for copy in before:
            copy.wait_recv()
        lines = part(core, block // 2)
        return send(gall.at[:, :, lines, :], gall.at[:, :, lines, :], sent_g.at[4, 0], came_g.at[4, 0], twin)

    def whole_factor(before):
        before.wait_recv()

        def cross(a, b):
            return gall[a, b - a - 1] if b - a <= 3 else gall[b, count - (b - a) - 1]

        last = count * block
        th[...] = jnp.zeros_like(th)
        tl[...] = jnp.zeros_like(tl)
        for k in range(count - 1, -1, -1):
            inner = halves(factors[k])
            lines, start = pl.ds(k * block, block), (k + 1) * block
            th[lines, lines], tl[lines, lines] = inner
            if start < last:
                rest = pl.ds(start, last - start)
                crossed = jnp.concatenate([cross(k, b) for b in range(k + 1, count)], axis=1)
                met = dot3(halves(crossed), (th[rest, rest], tl[rest, rest]), NN)
                th[lines, rest], tl[lines, rest] = halves(-dot3(inner, halves(met), NN))

    def project(c):
        whole = x.at[c]
        remote(whole, whole, sent_b.at[c], came_b.at[c], (row, col)).wait_recv()
        xh[...], xl[...] = halves(x[c])

        def two(p, carry):
            pair = pl.ds(p * 2, 2)
            right = [ref[pair].reshape(2 * block, piece) for ref in (vh, vl)]
            both = dot3((xh[...], xl[...]), right, NT)
            proj[c, p * 2] = both[:, :block]
            proj[c, p * 2 + 1] = both[:, block:]
            return carry

        lax.fori_loop(0, count // 2, two, 0)
        half = proj.shape[2] // 2
        return [
            send(proj.at[c, :, part(1 - core, half), :], r1.at[c], sent_p.at[c, 0], came_p.at[c, 0], twin)
        ]

    def sum_core(c, before):
        before[0].wait_recv()
        half = proj.shape[2] // 2
        r1[c] = r1[c] + proj[c, :, part(core, half), :]
        return [
            send(
                r1.at[c, :, part((y + k) % 4, half // 4), :], r2.at[c, k - 1],
                sent_p.at[c, k], came_p.at[c, k], in_y(k),
            )
            for k in (1, 3, 2)
        ]

    def sum_y(c, before):
        for copy in before:
            copy.wait_recv()
        s2[c] = r1[c, :, part(y, 32), :] + r2[c, 0] + (r2[c, 1] + r2[c, 2])
        return [
            send(
                s2.at[c, :, part((zh + k) % 4, 8), :], r3.at[c, k - 1],
                sent_p.at[c, 3 + k], came_p.at[c, 3 + k], in_z(k),
            )
            for k in (1, 3, 2)
        ]

    def update(c, before):
        for copy in before:
            copy.wait_recv()
        total = s2[c, :, part(zh, 8), :] + r3[c, 0] + (r3[c, 1] + r3[c, 2])
        flat = jnp.concatenate([total[k] for k in range(count)], axis=1)
        value = dot3(halves(flat), (th[...], tl[...]), NT)
        lines = part((core * 4 + y) * 4 + zh, 8)
        for k in range(count):
            upd[c, k, lines, :] = value[:, k * block : (k + 1) * block]
        ref = upd.at[c, :, lines, :]
        return [send(ref, ref, sent_p.at[c, 6 + k], came_p.at[c, 6 + k], in_z(k)) for k in (1, 3, 2)]

    def all_z(c, before):
        for copy in before:
            copy.wait_recv()
        ref = upd.at[c, :, part(core * 4 + y, 32), :]
        return [send(ref, ref, sent_p.at[c, 9 + k], came_p.at[c, 9 + k], in_y(k)) for k in (1, 3, 2)]

    def all_y(c, before):
        for copy in before:
            copy.wait_recv()
        ref = upd.at[c, :, part(core, 128), :]
        return [send(ref, ref, sent_p.at[c, 13], came_p.at[c, 13], twin)]

    def finish(c, before):
        before[0].wait_recv()
        flat = jnp.concatenate([upd[c, k] for k in range(count)], axis=1)
        uh[...], ul[...] = halves(flat)
        wide = 256

        def tile(t, carry):
            lanes = part(t, wide)
            right = [ref[:, :, lanes].reshape(count * block, wide) for ref in (vh, vl)]
            moved = x[c, :, lanes] - dot3((uh[...], ul[...]), right, NN)
            out[:, c, :, lanes] = moved.reshape(32, 8, wide)
            return carry

        lax.fori_loop(0, piece // wide, tile, 0)

    state = {}
    g = None
    for c in range(CHUNKS + 2):
        if c < CHUNKS:
            state[c] = project(c)
        if c == 0:
            g = g_col()
        if c == 1:
            whole_factor(g)
        if 0 <= c - 1 < CHUNKS:
            state[c - 1] = update(c - 1, state[c - 1])
        if c < CHUNKS:
            state[c] = sum_core(c, state[c])
        if c == 0:
            g = g_y(g)
        if 0 <= c - 2 < CHUNKS:
            state[c - 2] = all_z(c - 2, state[c - 2])
        if c < CHUNKS:
            state[c] = sum_y(c, state[c])
        if c == 0:
            g = g_core(g)
        if c + 2 < CHUNKS:
            second(c + 2)
        if 0 <= c - 2 < CHUNKS:
            state[c - 2] = all_y(c - 2, state[c - 2])
            finish(c - 2, state[c - 2])

    for c in range(CHUNKS):

        @pl.when(local)
        def _():
            some = x.at[c, pl.ds(0, x.shape[1] - 8), :]
            remote(some, some, sent_b.at[c], came_b.at[c], (row, col)).wait_send()

        @pl.when(jnp.logical_not(local))
        def _():
            remote(x.at[c], x.at[c], sent_b.at[c], came_b.at[c], (row, col)).wait_send()

    for copy in pending:
        copy.wait_send()


def on_device(vectors, reflectors, factors):
    count, block = factors.shape[:2]
    rows, length = vectors.shape
    piece = length // 32
    lot = rows * 32 // CHUNKS
    vmem = pltpu.VMEM
    dma = pltpu.SemaphoreType.DMA
    out = pl.pallas_call(
        kernel,
        out_shape=jax.ShapeDtypeStruct((32, CHUNKS, rows // CHUNKS, piece), F32),
        in_specs=[
            pl.BlockSpec(memory_space=pl.ANY),
            pl.BlockSpec(memory_space=pl.ANY),
            pl.BlockSpec(memory_space=vmem),
        ],
        out_specs=pl.BlockSpec(memory_space=vmem),
        scratch_shapes=[
            vmem((CHUNKS, lot, piece), F32),
            vmem((CHUNKS, 3, 8, 8 * piece), F32),
            vmem((count, block, piece), F32),
            vmem((count, block, piece), BF16),
            vmem((count, block, piece), BF16),
            vmem((lot, piece), BF16),
            vmem((lot, piece), BF16),
            vmem((lot, count * block), BF16),
            vmem((lot, count * block), BF16),
            vmem((CHUNKS, count, lot, block), F32),
            vmem((CHUNKS, count, lot // 2, block), F32),
            vmem((CHUNKS, 3, count, lot // 8, block), F32),
            vmem((CHUNKS, count, lot // 8, block), F32),
            vmem((CHUNKS, 3, count, lot // 32, block), F32),
            vmem((CHUNKS, count, lot, block), F32),
            vmem((3, block, block), F32),
            vmem((7, 3, block // 8, block), F32),
            vmem((3, block // 8, block), F32),
            vmem((3, 3, block // 8, block), F32),
            vmem((8, 3, block // 8, block), F32),
            vmem((count, 3, block, block), F32),
            vmem((count * block, count * block), BF16),
            vmem((count * block, count * block), BF16),
            dma((CHUNKS, 3)),
            dma((CHUNKS, 3)),
            dma((CHUNKS,)),
            dma((CHUNKS,)),
            dma((7,)),
            dma((7,)),
            dma,
            dma((5, 8)),
            dma((5, 8)),
            dma((CHUNKS, 14)),
            dma((CHUNKS, 14)),
        ],
        compiler_params=pltpu.CompilerParams(
            collective_id=1, has_side_effects=True, vmem_limit_bytes=60 * 2**20
        ),
    )(vectors, reflectors, factors)
    return out.reshape(rows * 32, piece)


def solution(mesh):
    placed = (P(("row", "col"), None), P(None, "col", "row"), P())
    return jax.shard_map(
        on_device, mesh=mesh, in_specs=placed, out_specs=P("col", "row"), check_vma=False
    )
```

```python
import jax
import jax.numpy as jnp
from jax import lax
from jax.experimental import pallas as pl
from jax.experimental.pallas import tpu as pltpu
from jax.sharding import PartitionSpec as P

F32 = jnp.float32
BF16 = jnp.bfloat16
MESH = pl.DeviceIdType.MESH
CHUNKS = 4
NT = (((1,), (1,)), ((), ()))
NN = (((1,), (0,)), ((), ()))


def halves(value):
    high = value.astype(BF16)
    return high, (value - high.astype(F32)).astype(BF16)


def dot3(left, right, dims):
    def one(a, b):
        return lax.dot_general(a, b, dims, preferred_element_type=F32)

    return one(left[0], right[0]) + (one(left[0], right[1]) + one(left[1], right[0]))


def part(index, size):
    return pl.ds(pl.multiple_of(index * size, size), size)


def kernel(
    vec, refl, factors, out,
    x, held, turned, passed, panels, vh, vl, xh, xl, uh, ul, proj, r1, r2, s2, r3, upd,
    gp, g1, gs, g2, gc, gall, th, tl,
    sent_a, came_a, sent_t, came_t, sent_r, came_r, sent_b, came_b, sent_v, came_v, own_v, sent_g, came_g, sent_p, came_p,
):
    row, col = lax.axis_index("row"), lax.axis_index("col")
    y, near = row // 8, row % 8
    zh, core = near // 2, near % 2
    far_x, zl = col // 2, col % 2
    upper = near // 4
    count, block, piece = panels.shape
    own = refl.shape[1]
    pending = []

    def at(y_, zh_, core_, col_):
        return (y_ * 8 + zh_ * 2 + core_, col_)

    def in_y(k):
        return at((y + k) % 4, zh, core, col)

    def in_z(k):
        return at(y, (zh + k) % 4, core, col)

    def in_x(k):
        return (row, ((far_x + k) % 4) * 2 + zl)

    twin = at(y, zh, 1 - core, col)

    def remote(src, dst, send_sem, recv_sem, device):
        return pltpu.make_async_remote_copy(
            src_ref=src, dst_ref=dst, send_sem=send_sem, recv_sem=recv_sem,
            device_id=device, device_id_type=MESH,
        )

    def send(*args):
        copy = remote(*args)
        copy.start()
        pending.append(copy)
        return copy

    barrier = pltpu.get_barrier_semaphore()
    greeted = []
    for w in range(8):
        greeted.append((y * 8 + w, far_x * 2 + upper))
        greeted.append((y * 8 + zl * 4 + w // 2, far_x * 2 + w % 2))
    for o in range(1, 8):
        greeted.append(at((y + o // 2) % 4, zh, (core + o) % 2, col))
        greeted.append((row, (col + o) % 8))
    for k in range(1, 4):
        greeted.append(in_z(k))
        greeted.append(at(y, (zh + k) % 4, 1 - core, col))
    for device in greeted:
        pl.semaphore_signal(barrier, inc=1, device_id=device, device_id_type=MESH)
    pl.semaphore_wait(barrier, len(greeted))

    first = {}
    for c in range(CHUNKS):
        for k in (1, 3, 2):
            first[c, k] = send(
                vec.at[pl.ds(c * 8, 8), part((y + k) % 4, 8 * piece)], held.at[c, k - 1],
                sent_a.at[c, k - 1], came_a.at[c, k - 1], in_y(k),
            )

    mine = panels.at[:, part(col, own), :]
    others = panels.at[:, part(far_x * 2 + 1 - zl, own), :]
    keep = pltpu.make_async_copy(refl, mine, own_v)
    keep.start()
    beside = send(refl, mine, sent_v.at[0], came_v.at[0], (row, far_x * 2 + 1 - zl))

    def turn(c):
        for k in (0, 1, 3, 2):
            if k:
                first[c, k].wait_recv()
            origin = (y - k) % 4
            source = held.at[c, k - 1] if k else vec.at[pl.ds(c * 8, 8), part(y, 8 * piece)]
            there = (origin - far_x) % 4
            target = turned.at[c, there]
            sem = came_t.at[c, there]

            @pl.when(origin == far_x)
            def _():
                pltpu.make_async_copy(source, target, sem).start()

            @pl.when(origin != far_x)
            def _():
                remote(source, target, sent_t.at[c], sem, (row, origin * 2 + zl)).start()

    local = zl == upper

    def slot(from_zh, k):
        return ((from_zh % 2) * 2 + core) * 8 + ((far_x - k) % 4) * 2 + zl

    def way(half):
        if half:
            return jnp.where(zh == 3, 1, 3)
        return jnp.where(zh == 0, 3, 1)

    def second(c):
        for k in (0, 1, 3, 2):
            remote(
                turned.at[c, k], turned.at[c, k], sent_t.at[c], came_t.at[c, k], (row, col)
            ).wait_recv()
            target = x.at[c, part(slot(zh, k), 8), :]
            for j in (2, 1, 3, 0):
                for flip in range(2):
                    to_zh, to_core = (zh + j) % 4, (core + flip) % 2
                    source = turned.at[c, k, :, part(to_zh * 2 + to_core, piece)]
                    device = at(y, to_zh, to_core, far_x * 2 + upper)
                    if j == 0 and flip == 0 or j == 2:

                        @pl.when(local)
                        def _():
                            if j == 0:
                                pltpu.make_async_copy(source, target, came_b.at[c]).start()
                            else:
                                remote(
                                    source, passed.at[c, flip, k], sent_b.at[c], came_r.at[c, flip],
                                    at(y, (zh + way(flip)) % 4, core, far_x * 2 + upper),
                                ).start()

                        @pl.when(jnp.logical_not(local))
                        def _():
                            remote(source, target, sent_b.at[c], came_b.at[c], device).start()

                    else:
                        remote(source, target, sent_b.at[c], came_b.at[c], device).start()

    from_zh = jnp.where(zl == 0, jnp.where(zh == 3, 0, 1), jnp.where(zh == 0, 3, 2))
    passes = (
        jnp.where(zl == 0, jnp.where(zh >= 2, 1, 0), jnp.where((zh + 1) % 4 <= 1, 1, 0)) == 1,
        jnp.where(zl == 0, jnp.where((zh + 1) % 4 <= 1, 1, 0), jnp.where(zh <= 1, 1, 0)) == 1,
    )

    def relay(c):
        for half in range(2):

            @pl.when(passes[half])
            def _():
                whole = passed.at[c, half]
                remote(whole, whole, sent_r.at[c, half], came_r.at[c, half], (row, col)).wait_recv()
                for k in (0, 1, 3, 2):
                    remote(
                        passed.at[c, half, k], x.at[c, part(slot(from_zh, k), 8), :],
                        sent_r.at[c, half], came_b.at[c],
                        at(y, (from_zh + 2) % 4, (core + half) % 2, col),
                    ).start()

    turn(0)
    second(0)
    from_x = [send(refl, mine, sent_v.at[k], came_v.at[k], in_x(k)) for k in (1, 3, 2)]
    turn(1)
    relay(0)
    turn(2)
    beside.wait_recv()
    from_z = [send(others, others, sent_v.at[3 + k], came_v.at[3 + k], in_x(k)) for k in (1, 3, 2)]
    second(1)
    relay(1)
    turn(3)
    second(2)
    relay(2)
    for copy in from_x + from_z:
        copy.wait_recv()
    keep.wait()
    for k in range(count):
        vh[k], vl[k] = halves(panels[k])

    line = col % count
    for d in range(1, 4):
        other = (line + d) % count
        low, high = jnp.minimum(line, other), jnp.maximum(line, other)
        gp[d - 1] = dot3((vh[low], vl[low]), (vh[high], vl[high]), NT)
    lot = block // 8
    step_1 = []
    for o in range(1, 8):
        to_y, to_core = (y + o // 2) % 4, (core + o) % 2
        step_1.append(
            send(
                gp.at[:, part(to_core * 4 + to_y, lot), :], g1.at[o - 1],
                sent_g.at[0, o], came_g.at[0, o], at(to_y, zh, to_core, col),
            )
        )
    def g_sum():
        for copy in step_1:
            copy.wait_recv()
        total = gp[:, part(core * 4 + y, lot), :]
        for o in range(7):
            total = total + g1[o]
        gs[...] = total
        return [send(gs, g2.at[k - 1], sent_g.at[1, k], came_g.at[1, k], in_z(k)) for k in (1, 3, 2)]

    def g_col(before):
        for copy in before:
            copy.wait_recv()
        gc[col] = gs[...] + g2[0] + (g2[1] + g2[2])
        return [
            send(gc.at[col], gc.at[col], sent_g.at[2, k], came_g.at[2, k], (row, (col + k) % 8))
            for k in range(1, 8)
        ]

    def g_y(before):
        for copy in before:
            copy.wait_recv()
        lines = part(core * 4 + y, lot)
        gall[:, :, lines, :] = gc[pl.ds(0, count)]
        return [
            send(
                gc.at[pl.ds(0, count)], gall.at[:, :, lines, :],
                sent_g.at[3, k], came_g.at[3, k], in_y(k),
            )
            for k in (1, 3, 2)
        ]

    def g_core(before):
        for copy in before:
            copy.wait_recv()
        lines = part(core, block // 2)
        return send(gall.at[:, :, lines, :], gall.at[:, :, lines, :], sent_g.at[4, 0], came_g.at[4, 0], twin)

    def whole_factor(before):
        before.wait_recv()

        def cross(a, b):
            return gall[a, b - a - 1] if b - a <= 3 else gall[b, count - (b - a) - 1]

        last = count * block
        th[...] = jnp.zeros_like(th)
        tl[...] = jnp.zeros_like(tl)
        for k in range(count - 1, -1, -1):
            inner = halves(factors[k])
            lines, start = pl.ds(k * block, block), (k + 1) * block
            th[lines, lines], tl[lines, lines] = inner
            if start < last:
                rest = pl.ds(start, last - start)
                crossed = jnp.concatenate([cross(k, b) for b in range(k + 1, count)], axis=1)
                met = dot3(halves(crossed), (th[rest, rest], tl[rest, rest]), NN)
                th[lines, rest], tl[lines, rest] = halves(-dot3(inner, halves(met), NN))

    def project(c):
        whole = x.at[c]
        remote(whole, whole, sent_b.at[c], came_b.at[c], (row, col)).wait_recv()
        xh[...], xl[...] = halves(x[c])

        def two(p, carry):
            pair = pl.ds(p * 2, 2)
            right = [ref[pair].reshape(2 * block, piece) for ref in (vh, vl)]
            both = dot3((xh[...], xl[...]), right, NT)
            proj[c, p * 2] = both[:, :block]
            proj[c, p * 2 + 1] = both[:, block:]
            return carry

        lax.fori_loop(0, count // 2, two, 0)
        half = proj.shape[2] // 2
        return [
            send(proj.at[c, :, part(1 - core, half), :], r1.at[c], sent_p.at[c, 0], came_p.at[c, 0], twin)
        ]

    def sum_core(c, before):
        before[0].wait_recv()
        half = proj.shape[2] // 2
        r1[c] = r1[c] + proj[c, :, part(core, half), :]
        return [
            send(
                r1.at[c, :, part((y + k) % 4, half // 4), :], r2.at[c, k - 1],
                sent_p.at[c, k], came_p.at[c, k], in_y(k),
            )
            for k in (1, 3, 2)
        ]

    def sum_y(c, before):
        for copy in before:
            copy.wait_recv()
        s2[c] = r1[c, :, part(y, 32), :] + r2[c, 0] + (r2[c, 1] + r2[c, 2])
        return [
            send(
                s2.at[c, :, part((zh + k) % 4, 8), :], r3.at[c, k - 1],
                sent_p.at[c, 3 + k], came_p.at[c, 3 + k], in_z(k),
            )
            for k in (1, 3, 2)
        ]

    def update(c, before):
        for copy in before:
            copy.wait_recv()
        total = s2[c, :, part(zh, 8), :] + r3[c, 0] + (r3[c, 1] + r3[c, 2])
        flat = jnp.concatenate([total[k] for k in range(count)], axis=1)
        value = dot3(halves(flat), (th[...], tl[...]), NT)
        lines = part((core * 4 + y) * 4 + zh, 8)
        for k in range(count):
            upd[c, k, lines, :] = value[:, k * block : (k + 1) * block]
        ref = upd.at[c, :, lines, :]
        return [send(ref, ref, sent_p.at[c, 6 + k], came_p.at[c, 6 + k], in_z(k)) for k in (1, 3, 2)]

    def all_z(c, before):
        for copy in before:
            copy.wait_recv()
        ref = upd.at[c, :, part(core * 4 + y, 32), :]
        return [send(ref, ref, sent_p.at[c, 9 + k], came_p.at[c, 9 + k], in_y(k)) for k in (1, 3, 2)]

    def all_y(c, before):
        for copy in before:
            copy.wait_recv()
        ref = upd.at[c, :, part(core, 128), :]
        return [send(ref, ref, sent_p.at[c, 13], came_p.at[c, 13], twin)]

    def finish(c, before):
        before[0].wait_recv()
        flat = jnp.concatenate([upd[c, k] for k in range(count)], axis=1)
        uh[...], ul[...] = halves(flat)
        wide = 256

        def tile(t, carry):
            lanes = part(t, wide)
            right = [ref[:, :, lanes].reshape(count * block, wide) for ref in (vh, vl)]
            moved = x[c, :, lanes] - dot3((uh[...], ul[...]), right, NN)
            out[:, c, :, lanes] = moved.reshape(32, 8, wide)
            return carry

        lax.fori_loop(0, piece // wide, tile, 0)

    at_0, at_1 = project(0), project(1)
    g = g_sum()
    at_0, at_1 = sum_core(0, at_0), sum_core(1, at_1)
    at_0, at_1 = sum_y(0, at_0), sum_y(1, at_1)
    g = g_col(g)
    second(3)
    relay(3)
    at_2 = project(2)
    g = g_y(g)
    at_2 = sum_core(2, at_2)
    g = g_core(g)
    at_2 = sum_y(2, at_2)
    whole_factor(g)
    at_0, at_1 = update(0, at_0), update(1, at_1)
    at_3 = project(3)
    at_2 = update(2, at_2)
    at_3 = sum_core(3, at_3)
    at_0, at_1 = all_z(0, at_0), all_z(1, at_1)
    at_3 = sum_y(3, at_3)
    at_2 = all_z(2, at_2)
    at_0, at_1 = all_y(0, at_0), all_y(1, at_1)
    at_3 = update(3, at_3)
    finish(0, at_0)
    at_3 = all_z(3, at_3)
    at_2 = all_y(2, at_2)
    finish(1, at_1)
    at_3 = all_y(3, at_3)
    finish(2, at_2)
    finish(3, at_3)

    for c in range(CHUNKS):
        three = turned.at[c, pl.ds(0, 3)]
        remote(three, three, sent_t.at[c], came_t.at[c, 0], (row, col)).wait_send()

        @pl.when(local)
        def _():
            some = x.at[c, pl.ds(0, x.shape[1] - 32), :]
            remote(some, some, sent_b.at[c], came_b.at[c], (row, col)).wait_send()

        @pl.when(jnp.logical_not(local))
        def _():
            remote(x.at[c], x.at[c], sent_b.at[c], came_b.at[c], (row, col)).wait_send()

        for half in range(2):

            @pl.when(passes[half])
            def _():
                whole = passed.at[c, half]
                remote(whole, whole, sent_r.at[c, half], came_r.at[c, half], (row, col)).wait_send()

    for copy in pending:
        copy.wait_send()


def on_device(vectors, reflectors, factors):
    count, block = factors.shape[:2]
    rows, length = vectors.shape
    piece = length // 32
    lot = rows * 32 // CHUNKS
    vmem = pltpu.VMEM
    dma = pltpu.SemaphoreType.DMA
    out = pl.pallas_call(
        kernel,
        out_shape=vmem((32, CHUNKS, rows // CHUNKS, piece), F32),
        in_specs=[
            pl.BlockSpec(memory_space=pl.ANY),
            pl.BlockSpec(memory_space=pl.ANY),
            pl.BlockSpec(memory_space=vmem),
        ],
        out_specs=pl.BlockSpec(memory_space=vmem),
        scratch_shapes=[
            vmem((CHUNKS, lot, piece), F32),
            vmem((CHUNKS, 3, 8, 8 * piece), F32),
            vmem((CHUNKS, 4, 8, 8 * piece), F32),
            vmem((CHUNKS, 2, 4, 8, piece), F32),
            vmem((count, block, piece), F32),
            vmem((count, block, piece), BF16),
            vmem((count, block, piece), BF16),
            vmem((lot, piece), BF16),
            vmem((lot, piece), BF16),
            vmem((lot, count * block), BF16),
            vmem((lot, count * block), BF16),
            vmem((CHUNKS, count, lot, block), F32),
            vmem((CHUNKS, count, lot // 2, block), F32),
            vmem((CHUNKS, 3, count, lot // 8, block), F32),
            vmem((CHUNKS, count, lot // 8, block), F32),
            vmem((CHUNKS, 3, count, lot // 32, block), F32),
            vmem((CHUNKS, count, lot, block), F32),
            vmem((3, block, block), F32),
            vmem((7, 3, block // 8, block), F32),
            vmem((3, block // 8, block), F32),
            vmem((3, 3, block // 8, block), F32),
            vmem((8, 3, block // 8, block), F32),
            vmem((count, 3, block, block), F32),
            vmem((count * block, count * block), BF16),
            vmem((count * block, count * block), BF16),
            dma((CHUNKS, 3)),
            dma((CHUNKS, 3)),
            dma((CHUNKS,)),
            dma((CHUNKS, 4)),
            dma((CHUNKS, 2)),
            dma((CHUNKS, 2)),
            dma((CHUNKS,)),
            dma((CHUNKS,)),
            dma((7,)),
            dma((7,)),
            dma,
            dma((5, 8)),
            dma((5, 8)),
            dma((CHUNKS, 14)),
            dma((CHUNKS, 14)),
        ],
        compiler_params=pltpu.CompilerParams(
            collective_id=1, has_side_effects=True, vmem_limit_bytes=52 * 2**20
        ),
    )(vectors, reflectors, factors)
    return out.reshape(rows * 32, piece)


def solution(mesh):
    placed = (P(("row", "col"), None), P(None, "col", "row"), P())
    return jax.shard_map(
        on_device, mesh=mesh, in_specs=placed, out_specs=P("col", "row"), check_vma=False
    )
```

```python
import jax
import jax.numpy as jnp
from jax import lax
from jax.experimental import pallas as pl
from jax.experimental.pallas import tpu as pltpu
from jax.sharding import PartitionSpec as P

F32 = jnp.float32
BF16 = jnp.bfloat16
MESH = pl.DeviceIdType.MESH
CHUNKS = 4
LAST = CHUNKS - 1
NT = (((1,), (1,)), ((), ()))
NN = (((1,), (0,)), ((), ()))


def halves(value):
    high = value.astype(BF16)
    return high, (value - high.astype(F32)).astype(BF16)


def dot3(left, right, dims):
    def one(a, b):
        return lax.dot_general(a, b, dims, preferred_element_type=F32)

    return one(left[0], right[0]) + (one(left[0], right[1]) + one(left[1], right[0]))


def part(index, size):
    return pl.ds(pl.multiple_of(index * size, size), size)


def kernel(
    vec, refl, factors, out,
    x, held, turned, passed, early, risen, passed_early, panels, vh, vl, xh, xl, uh, ul, proj, r1, r2, s2, r3, upd,
    gp, g1, gs, g2, gc, gall, th, tl,
    sent_a, came_a, sent_t, came_t, sent_r, came_r, sent_b, came_b,
    sent_e, came_e, sent_pe, came_pe, sent_u, came_u, sent_v, came_v, own_v, sent_g, came_g, sent_p, came_p,
):
    row, col = lax.axis_index("row"), lax.axis_index("col")
    y, near = row // 8, row % 8
    zh, core = near // 2, near % 2
    far_x, zl = col // 2, col % 2
    upper = near // 4
    count, block, piece = panels.shape
    own = refl.shape[1]
    pending = []

    def at(y_, zh_, core_, col_):
        return (y_ * 8 + zh_ * 2 + core_, col_)

    def in_y(k):
        return at((y + k) % 4, zh, core, col)

    def in_z(k):
        return at(y, (zh + k) % 4, core, col)

    def in_x(k):
        return (row, ((far_x + k) % 4) * 2 + zl)

    twin = at(y, zh, 1 - core, col)

    def remote(src, dst, send_sem, recv_sem, device):
        return pltpu.make_async_remote_copy(
            src_ref=src, dst_ref=dst, send_sem=send_sem, recv_sem=recv_sem,
            device_id=device, device_id_type=MESH,
        )

    def send(*args):
        copy = remote(*args)
        copy.start()
        pending.append(copy)
        return copy

    barrier = pltpu.get_barrier_semaphore()
    greeted = []
    for w in range(8):
        greeted.append((y * 8 + w, far_x * 2 + upper))
        greeted.append((y * 8 + zl * 4 + w // 2, far_x * 2 + w % 2))
    for o in range(1, 8):
        greeted.append(at((y + o // 2) % 4, zh, (core + o) % 2, col))
        greeted.append((row, (col + o) % 8))
    for k in range(1, 4):
        greeted.append(in_z(k))
        greeted.append(at(y, (zh + k) % 4, 1 - core, col))
        greeted.append((row + 1 - 2 * core, ((far_x + k) % 4) * 2 + zl))
    for device in greeted:
        pl.semaphore_signal(barrier, inc=1, device_id=device, device_id_type=MESH)
    pl.semaphore_wait(barrier, len(greeted))

    first = {}

    def begin(c):
        for k in (1, 3, 2):
            first[c, k] = send(
                vec.at[pl.ds(c * 8, 8), part((y + k) % 4, 8 * piece)], held.at[c, k - 1],
                sent_a.at[c, k - 1], came_a.at[c, k - 1], in_y(k),
            )

    begin(0)

    mine = panels.at[:, part(col, own), :]
    others = panels.at[:, part(far_x * 2 + 1 - zl, own), :]
    keep = pltpu.make_async_copy(refl, mine, own_v)
    keep.start()
    beside = send(refl, mine, sent_v.at[0], came_v.at[0], (row, far_x * 2 + 1 - zl))

    def turn(c):
        for k in (0, 1, 3, 2):
            if k:
                first[c, k].wait_recv()
            origin = (y - k) % 4
            source = held.at[c, k - 1] if k else vec.at[pl.ds(c * 8, 8), part(y, 8 * piece)]
            there = (origin - far_x) % 4
            target = turned.at[c, there]
            sem = came_t.at[c, there]

            @pl.when(origin == far_x)
            def _():
                pltpu.make_async_copy(source, target, sem).start()

            @pl.when(origin != far_x)
            def _():
                remote(source, target, sent_t.at[c], sem, (row, origin * 2 + zl)).start()

    local = zl == upper

    def slot(from_zh, k):
        return ((from_zh % 2) * 2 + core) * 8 + ((far_x - k) % 4) * 2 + zl

    def way(half):
        if half:
            return jnp.where(zh == 3, 1, 3)
        return jnp.where(zh == 0, 3, 1)

    def second(c, steps=(0, 1, 3, 2)):
        for k in steps:
            remote(
                turned.at[c, k], turned.at[c, k], sent_t.at[c], came_t.at[c, k], (row, col)
            ).wait_recv()
            target = x.at[c, part(slot(zh, k), 8), :]
            for j in (2, 1, 3, 0):
                for flip in range(2):
                    to_zh, to_core = (zh + j) % 4, (core + flip) % 2
                    source = turned.at[c, k, :, part(to_zh * 2 + to_core, piece)]
                    device = at(y, to_zh, to_core, far_x * 2 + upper)
                    if j == 0 and flip == 0 or j == 2:

                        @pl.when(local)
                        def _():
                            if j == 0:
                                pltpu.make_async_copy(source, target, came_b.at[c]).start()
                            else:
                                remote(
                                    source, passed.at[c, flip, k], sent_b.at[c], came_r.at[c, flip],
                                    at(y, (zh + way(flip)) % 4, core, far_x * 2 + upper),
                                ).start()

                        @pl.when(jnp.logical_not(local))
                        def _():
                            remote(source, target, sent_b.at[c], came_b.at[c], device).start()

                    else:
                        remote(source, target, sent_b.at[c], came_b.at[c], device).start()

    from_zh = jnp.where(zl == 0, jnp.where(zh == 3, 0, 1), jnp.where(zh == 0, 3, 2))
    passes = (
        jnp.where(zl == 0, jnp.where(zh >= 2, 1, 0), jnp.where((zh + 1) % 4 <= 1, 1, 0)) == 1,
        jnp.where(zl == 0, jnp.where((zh + 1) % 4 <= 1, 1, 0), jnp.where(zh <= 1, 1, 0)) == 1,
    )

    def relay(c):
        for half in range(2):

            @pl.when(passes[half])
            def _():
                whole = passed.at[c, half]
                remote(whole, whole, sent_r.at[c, half], came_r.at[c, half], (row, col)).wait_recv()
                for k in (0, 1, 3, 2):
                    remote(
                        passed.at[c, half, k], x.at[c, part(slot(from_zh, k), 8), :],
                        sent_r.at[c, half], came_b.at[c],
                        at(y, (from_zh + 2) % 4, (core + half) % 2, col),
                    ).start()

    def early_z():
        for j in (2, 1, 3, 0):
            for k in range(4):
                to_y, to_zh = (y + k) % 4, (zh + j) % 4
                source = vec.at[pl.ds(LAST * 8, 8), part(to_y * 4 + to_zh, 2 * piece)]
                target = early.at[to_y, (zh % 2) * 2 + zl]
                device = at(y, to_zh, core, far_x * 2 + upper)
                if j % 2:
                    remote(source, target, sent_e, came_e, device).start()
                else:

                    @pl.when(local)
                    def _():
                        if j == 0:
                            pltpu.make_async_copy(source, target, came_e).start()
                        else:
                            remote(
                                source, passed_early.at[k // 2, k % 2], sent_e, came_pe.at[k // 2],
                                at(y, (zh + way(k // 2)) % 4, core, far_x * 2 + upper),
                            ).start()

                    @pl.when(jnp.logical_not(local))
                    def _():
                        remote(source, target, sent_e, came_e, device).start()

    def early_relay():
        for half in range(2):

            @pl.when(passes[half])
            def _():
                whole = passed_early.at[half]
                remote(whole, whole, sent_pe.at[half], came_pe.at[half], (row, col)).wait_recv()
                for i in range(2):
                    remote(
                        passed_early.at[half, i], early.at[(y + half * 2 + i) % 4, (from_zh % 2) * 2 + zl],
                        sent_pe.at[half], came_e, at(y, (from_zh + 2) % 4, core, col),
                    ).start()

    def early_y():
        remote(early, early, sent_e, came_e, (row, col)).wait_recv()
        return {
            k: send(
                early.at[(y + k) % 4], risen.at[k - 1], sent_u.at[k - 1], came_u.at[k - 1], in_y(k)
            )
            for k in (1, 3, 2)
        }

    def early_x(before):
        for k in (0, 1, 3, 2):
            if k:
                before[k].wait_recv()
            origin = (y - k) % 4
            for q in range(4):
                for flip in range(2):
                    to_core = (core + flip) % 2
                    lanes = part(to_core, piece)
                    source = risen.at[k - 1, q, :, lanes] if k else early.at[y, q, :, lanes]
                    place = (q // 2 * 2 + core) * 8 + far_x * 2 + q % 2
                    target = x.at[LAST, part(place, 8), :]
                    there = remote(
                        source, target, sent_b.at[LAST], came_b.at[LAST], at(y, zh, to_core, origin * 2 + zl)
                    )
                    if flip:
                        there.start()
                    else:

                        @pl.when(origin == far_x)
                        def _():
                            pltpu.make_async_copy(source, target, came_b.at[LAST]).start()

                        @pl.when(origin != far_x)
                        def _():
                            there.start()

    early_z()
    begin(1)
    begin(2)
    turn(0)
    from_x = [send(refl, mine, sent_v.at[k], came_v.at[k], in_x(k)) for k in (1, 3, 2)]
    early_relay()
    second(0)
    beside.wait_recv()
    from_z = [send(others, others, sent_v.at[3 + k], came_v.at[3 + k], in_x(k)) for k in (1, 3, 2)]
    turn(1)
    relay(0)
    turn(2)
    rising = early_y()
    for copy in from_x + from_z:
        copy.wait_recv()
    keep.wait()
    for k in range(count):
        vh[k], vl[k] = halves(panels[k])

    line = col % count
    for d in range(1, 4):
        other = (line + d) % count
        low, high = jnp.minimum(line, other), jnp.maximum(line, other)
        gp[d - 1] = dot3((vh[low], vl[low]), (vh[high], vl[high]), NT)
    lot = block // 8
    step_1 = []
    for o in range(1, 8):
        to_y, to_core = (y + o // 2) % 4, (core + o) % 2
        step_1.append(
            send(
                gp.at[:, part(to_core * 4 + to_y, lot), :], g1.at[o - 1],
                sent_g.at[0, o], came_g.at[0, o], at(to_y, zh, to_core, col),
            )
        )
    def g_sum():
        for copy in step_1:
            copy.wait_recv()
        total = gp[:, part(core * 4 + y, lot), :]
        for o in range(7):
            total = total + g1[o]
        gs[...] = total
        return [send(gs, g2.at[k - 1], sent_g.at[1, k], came_g.at[1, k], in_z(k)) for k in (1, 3, 2)]

    def g_col(before):
        for copy in before:
            copy.wait_recv()
        gc[col] = gs[...] + g2[0] + (g2[1] + g2[2])
        return [
            send(gc.at[col], gc.at[col], sent_g.at[2, k], came_g.at[2, k], (row, (col + k) % 8))
            for k in range(1, 8)
        ]

    def g_y(before):
        for copy in before:
            copy.wait_recv()
        lines = part(core * 4 + y, lot)
        gall[:, :, lines, :] = gc[pl.ds(0, count)]
        return [
            send(
                gc.at[pl.ds(0, count)], gall.at[:, :, lines, :],
                sent_g.at[3, k], came_g.at[3, k], in_y(k),
            )
            for k in (1, 3, 2)
        ]

    def g_core(before):
        for copy in before:
            copy.wait_recv()
        lines = part(core, block // 2)
        return send(gall.at[:, :, lines, :], gall.at[:, :, lines, :], sent_g.at[4, 0], came_g.at[4, 0], twin)

    def whole_factor(before):
        before.wait_recv()

        def cross(a, b):
            return gall[a, b - a - 1] if b - a <= 3 else gall[b, count - (b - a) - 1]

        last = count * block
        th[...] = jnp.zeros_like(th)
        tl[...] = jnp.zeros_like(tl)
        for k in range(count - 1, -1, -1):
            inner = halves(factors[k])
            lines, start = pl.ds(k * block, block), (k + 1) * block
            th[lines, lines], tl[lines, lines] = inner
            if start < last:
                rest = pl.ds(start, last - start)
                crossed = jnp.concatenate([cross(k, b) for b in range(k + 1, count)], axis=1)
                met = dot3(halves(crossed), (th[rest, rest], tl[rest, rest]), NN)
                th[lines, rest], tl[lines, rest] = halves(-dot3(inner, halves(met), NN))

    def project(c):
        whole = x.at[c]
        remote(whole, whole, sent_b.at[c], came_b.at[c], (row, col)).wait_recv()
        xh[...], xl[...] = halves(x[c])

        def two(p, carry):
            pair = pl.ds(p * 2, 2)
            right = [ref[pair].reshape(2 * block, piece) for ref in (vh, vl)]
            both = dot3((xh[...], xl[...]), right, NT)
            proj[c, p * 2] = both[:, :block]
            proj[c, p * 2 + 1] = both[:, block:]
            return carry

        lax.fori_loop(0, count // 2, two, 0)
        half = proj.shape[2] // 2
        return [
            send(proj.at[c, :, part(1 - core, half), :], r1.at[c], sent_p.at[c, 0], came_p.at[c, 0], twin)
        ]

    def sum_core(c, before):
        before[0].wait_recv()
        half = proj.shape[2] // 2
        r1[c] = r1[c] + proj[c, :, part(core, half), :]
        return [
            send(
                r1.at[c, :, part((y + k) % 4, half // 4), :], r2.at[c, k - 1],
                sent_p.at[c, k], came_p.at[c, k], in_y(k),
            )
            for k in (1, 3, 2)
        ]

    def sum_y(c, before):
        for copy in before:
            copy.wait_recv()
        s2[c] = r1[c, :, part(y, 32), :] + r2[c, 0] + (r2[c, 1] + r2[c, 2])
        return [
            send(
                s2.at[c, :, part((zh + k) % 4, 8), :], r3.at[c, k - 1],
                sent_p.at[c, 3 + k], came_p.at[c, 3 + k], in_z(k),
            )
            for k in (1, 3, 2)
        ]

    def update(c, before):
        for copy in before:
            copy.wait_recv()
        total = s2[c, :, part(zh, 8), :] + r3[c, 0] + (r3[c, 1] + r3[c, 2])
        flat = jnp.concatenate([total[k] for k in range(count)], axis=1)
        value = dot3(halves(flat), (th[...], tl[...]), NT)
        lines = part((core * 4 + y) * 4 + zh, 8)
        for k in range(count):
            upd[c, k, lines, :] = value[:, k * block : (k + 1) * block]
        ref = upd.at[c, :, lines, :]
        return [send(ref, ref, sent_p.at[c, 6 + k], came_p.at[c, 6 + k], in_z(k)) for k in (1, 3, 2)]

    def all_z(c, before):
        for copy in before:
            copy.wait_recv()
        ref = upd.at[c, :, part(core * 4 + y, 32), :]
        return [send(ref, ref, sent_p.at[c, 9 + k], came_p.at[c, 9 + k], in_y(k)) for k in (1, 3, 2)]

    def all_y(c, before):
        for copy in before:
            copy.wait_recv()
        ref = upd.at[c, :, part(core, 128), :]
        return [send(ref, ref, sent_p.at[c, 13], came_p.at[c, 13], twin)]

    def finish(c, before):
        before[0].wait_recv()
        flat = jnp.concatenate([upd[c, k] for k in range(count)], axis=1)
        uh[...], ul[...] = halves(flat)
        wide = 256

        def tile(t, carry):
            lanes = part(t, wide)
            right = [ref[:, :, lanes].reshape(count * block, wide) for ref in (vh, vl)]
            moved = x[c, :, lanes] - dot3((uh[...], ul[...]), right, NN)
            out[:, c, :, lanes] = moved.reshape(32, 8, wide)
            return carry

        lax.fori_loop(0, piece // wide, tile, 0)

    at_0 = project(0)
    g = g_sum()
    second(1, (0, 1))
    g = g_col(g)
    second(1, (3, 2))
    at_0 = sum_core(0, at_0)
    relay(1)
    at_0 = sum_y(0, at_0)
    early_x(rising)
    second(2)
    g = g_y(g)
    at_3 = project(3)
    g = g_core(g)
    at_1 = project(1)
    at_3 = sum_core(3, at_3)
    whole_factor(g)
    at_0 = update(0, at_0)
    at_1 = sum_core(1, at_1)
    at_3 = sum_y(3, at_3)
    at_1 = sum_y(1, at_1)
    relay(2)
    at_2 = project(2)
    at_3 = update(3, at_3)
    at_2 = sum_core(2, at_2)
    at_1 = update(1, at_1)
    at_0 = all_z(0, at_0)
    at_3 = all_z(3, at_3)
    at_2 = sum_y(2, at_2)
    at_1 = all_z(1, at_1)
    at_0 = all_y(0, at_0)
    at_2 = update(2, at_2)
    at_3 = all_y(3, at_3)
    finish(0, at_0)
    at_2 = all_z(2, at_2)
    at_1 = all_y(1, at_1)
    finish(3, at_3)
    at_2 = all_y(2, at_2)
    finish(1, at_1)
    finish(2, at_2)

    for c in range(LAST):
        three = turned.at[c, pl.ds(0, 3)]
        remote(three, three, sent_t.at[c], came_t.at[c, 0], (row, col)).wait_send()

        @pl.when(local)
        def _():
            some = x.at[c, pl.ds(0, x.shape[1] - 32), :]
            remote(some, some, sent_b.at[c], came_b.at[c], (row, col)).wait_send()

        @pl.when(jnp.logical_not(local))
        def _():
            remote(x.at[c], x.at[c], sent_b.at[c], came_b.at[c], (row, col)).wait_send()

        for half in range(2):

            @pl.when(passes[half])
            def _():
                whole = passed.at[c, half]
                remote(whole, whole, sent_r.at[c, half], came_r.at[c, half], (row, col)).wait_send()

    sent = x.at[LAST, pl.ds(0, x.shape[1] - 32), :]
    remote(sent, sent, sent_b.at[LAST], came_b.at[LAST], (row, col)).wait_send()

    @pl.when(local)
    def _():
        some = early.at[pl.ds(0, 3)]
        remote(some, some, sent_e, came_e, (row, col)).wait_send()

    @pl.when(jnp.logical_not(local))
    def _():
        remote(early, early, sent_e, came_e, (row, col)).wait_send()

    for half in range(2):

        @pl.when(passes[half])
        def _():
            whole = passed_early.at[half]
            remote(whole, whole, sent_pe.at[half], came_pe.at[half], (row, col)).wait_send()

    for copy in pending:
        copy.wait_send()


def on_device(vectors, reflectors, factors):
    count, block = factors.shape[:2]
    rows, length = vectors.shape
    piece = length // 32
    lot = rows * 32 // CHUNKS
    vmem = pltpu.VMEM
    dma = pltpu.SemaphoreType.DMA
    out = pl.pallas_call(
        kernel,
        out_shape=vmem((32, CHUNKS, rows // CHUNKS, piece), F32),
        in_specs=[
            pl.BlockSpec(memory_space=pl.ANY),
            pl.BlockSpec(memory_space=pl.ANY),
            pl.BlockSpec(memory_space=vmem),
        ],
        out_specs=pl.BlockSpec(memory_space=vmem),
        scratch_shapes=[
            vmem((CHUNKS, lot, piece), F32),
            vmem((LAST, 3, 8, 8 * piece), F32),
            vmem((LAST, 4, 8, 8 * piece), F32),
            vmem((LAST, 2, 4, 8, piece), F32),
            vmem((4, 4, 8, 2 * piece), F32),
            vmem((3, 4, 8, 2 * piece), F32),
            vmem((2, 2, 8, 2 * piece), F32),
            vmem((count, block, piece), F32),
            vmem((count, block, piece), BF16),
            vmem((count, block, piece), BF16),
            vmem((lot, piece), BF16),
            vmem((lot, piece), BF16),
            vmem((lot, count * block), BF16),
            vmem((lot, count * block), BF16),
            vmem((CHUNKS, count, lot, block), F32),
            vmem((CHUNKS, count, lot // 2, block), F32),
            vmem((CHUNKS, 3, count, lot // 8, block), F32),
            vmem((CHUNKS, count, lot // 8, block), F32),
            vmem((CHUNKS, 3, count, lot // 32, block), F32),
            vmem((CHUNKS, count, lot, block), F32),
            vmem((3, block, block), F32),
            vmem((7, 3, block // 8, block), F32),
            vmem((3, block // 8, block), F32),
            vmem((3, 3, block // 8, block), F32),
            vmem((8, 3, block // 8, block), F32),
            vmem((count, 3, block, block), F32),
            vmem((count * block, count * block), BF16),
            vmem((count * block, count * block), BF16),
            dma((CHUNKS, 3)),
            dma((CHUNKS, 3)),
            dma((CHUNKS,)),
            dma((CHUNKS, 4)),
            dma((CHUNKS, 2)),
            dma((CHUNKS, 2)),
            dma((CHUNKS,)),
            dma((CHUNKS,)),
            dma,
            dma,
            dma((2,)),
            dma((2,)),
            dma((3,)),
            dma((3,)),
            dma((7,)),
            dma((7,)),
            dma,
            dma((5, 8)),
            dma((5, 8)),
            dma((CHUNKS, 14)),
            dma((CHUNKS, 14)),
        ],
        compiler_params=pltpu.CompilerParams(
            collective_id=1, has_side_effects=True, vmem_limit_bytes=52 * 2**20
        ),
    )(vectors, reflectors, factors)
    return out.reshape(rows * 32, piece)


def solution(mesh):
    placed = (P(("row", "col"), None), P(None, "col", "row"), P())
    return jax.shard_map(
        on_device, mesh=mesh, in_specs=placed, out_specs=P("col", "row"), check_vma=False
    )
```

```python
import jax
import jax.numpy as jnp
from jax import lax
from jax.experimental import pallas as pl
from jax.experimental.pallas import tpu as pltpu
from jax.sharding import PartitionSpec as P

F32 = jnp.float32
BF16 = jnp.bfloat16
MESH = pl.DeviceIdType.MESH
CHUNKS = 4
LAST = CHUNKS - 1
NT = (((1,), (1,)), ((), ()))
NN = (((1,), (0,)), ((), ()))


def halves(value):
    high = value.astype(BF16)
    return high, (value - high.astype(F32)).astype(BF16)


def dot3(left, right, dims):
    def one(a, b):
        return lax.dot_general(a, b, dims, preferred_element_type=F32)

    return one(left[0], right[0]) + (one(left[0], right[1]) + one(left[1], right[0]))


def part(index, size):
    return pl.ds(pl.multiple_of(index * size, size), size)


def kernel(
    vec, refl, factors, out,
    x, held, turned, passed, early, risen, passed_early, panels, vh, vl, xh, xl, uh, ul, proj, r1, r2, s2, r3, upd,
    gp, g1, gs, g2, gc, gall, th, tl,
    sent_a, came_a, sent_t, came_t, sent_r, came_r, sent_b, came_b,
    sent_e, came_e, sent_pe, came_pe, sent_u, came_u, sent_v, came_v, own_v, sent_g, came_g, sent_p, came_p,
):
    row, col = lax.axis_index("row"), lax.axis_index("col")
    y, near = row // 8, row % 8
    zh, core = near // 2, near % 2
    far_x, zl = col // 2, col % 2
    upper = near // 4
    count, block, piece = panels.shape
    own = refl.shape[1]
    pending = []

    def at(y_, zh_, core_, col_):
        return (y_ * 8 + zh_ * 2 + core_, col_)

    def in_y(k):
        return at((y + k) % 4, zh, core, col)

    def in_z(k):
        return at(y, (zh + k) % 4, core, col)

    def in_x(k):
        return (row, ((far_x + k) % 4) * 2 + zl)

    twin = at(y, zh, 1 - core, col)

    def remote(src, dst, send_sem, recv_sem, device):
        return pltpu.make_async_remote_copy(
            src_ref=src, dst_ref=dst, send_sem=send_sem, recv_sem=recv_sem,
            device_id=device, device_id_type=MESH,
        )

    def send(*args):
        copy = remote(*args)
        copy.start()
        pending.append(copy)
        return copy

    barrier = pltpu.get_barrier_semaphore()
    greeted = []
    for w in range(8):
        greeted.append((y * 8 + w, far_x * 2 + upper))
        greeted.append((y * 8 + zl * 4 + w // 2, far_x * 2 + w % 2))
    for o in range(1, 8):
        greeted.append(at((y + o // 2) % 4, zh, (core + o) % 2, col))
        greeted.append((row, (col + o) % 8))
    for k in range(1, 4):
        greeted.append(in_z(k))
        greeted.append(at(y, (zh + k) % 4, 1 - core, col))
        greeted.append((row + 1 - 2 * core, ((far_x + k) % 4) * 2 + zl))
    for device in greeted:
        pl.semaphore_signal(barrier, inc=1, device_id=device, device_id_type=MESH)
    pl.semaphore_wait(barrier, len(greeted))

    first = {}

    def begin(c):
        for k in (1, 3, 2):
            first[c, k] = send(
                vec.at[pl.ds(c * 8, 8), part((y + k) % 4, 8 * piece)], held.at[c, k - 1],
                sent_a.at[c, k - 1], came_a.at[c, k - 1], in_y(k),
            )

    begin(0)

    mine = panels.at[:, part(col, own), :]
    others = panels.at[:, part(far_x * 2 + 1 - zl, own), :]
    keep = pltpu.make_async_copy(refl, mine, own_v)
    keep.start()
    beside = send(refl, mine, sent_v.at[0], came_v.at[0], (row, far_x * 2 + 1 - zl))

    def turn(c):
        for k in (0, 1, 3, 2):
            if k:
                first[c, k].wait_recv()
            origin = (y - k) % 4
            source = held.at[c, k - 1] if k else vec.at[pl.ds(c * 8, 8), part(y, 8 * piece)]
            there = (origin - far_x) % 4
            target = turned.at[c, there]
            sem = came_t.at[c, there]

            @pl.when(origin == far_x)
            def _():
                pltpu.make_async_copy(source, target, sem).start()

            @pl.when(origin != far_x)
            def _():
                remote(source, target, sent_t.at[c], sem, (row, origin * 2 + zl)).start()

    local = zl == upper

    def slot(from_zh, k):
        return ((from_zh % 2) * 2 + core) * 8 + ((far_x - k) % 4) * 2 + zl

    def way(half):
        if half:
            return jnp.where(zh == 3, 1, 3)
        return jnp.where(zh == 0, 3, 1)

    def second(c, steps=(0, 1, 3, 2), opposite=True):
        def go(k, j):
            target = x.at[c, part(slot(zh, k), 8), :]
            for flip in range(2):
                to_zh, to_core = (zh + j) % 4, (core + flip) % 2
                source = turned.at[c, k, :, part(to_zh * 2 + to_core, piece)]
                device = at(y, to_zh, to_core, far_x * 2 + upper)
                if j == 0 and flip == 0 or j == 2:

                    @pl.when(local)
                    def _():
                        if j == 0:
                            pltpu.make_async_copy(source, target, came_b.at[c]).start()
                        else:
                            remote(
                                source, passed.at[c, flip, k], sent_b.at[c], came_r.at[c, flip],
                                at(y, (zh + way(flip)) % 4, core, far_x * 2 + upper),
                            ).start()

                    @pl.when(jnp.logical_not(local))
                    def _():
                        remote(source, target, sent_b.at[c], came_b.at[c], device).start()

                else:
                    remote(source, target, sent_b.at[c], came_b.at[c], device).start()

        if opposite:
            for k in (0, 1, 3, 2):
                remote(
                    turned.at[c, k], turned.at[c, k], sent_t.at[c], came_t.at[c, k], (row, col)
                ).wait_recv()
                go(k, 2)
        for k in steps:
            for j in (1, 3, 0):
                go(k, j)

    from_zh = jnp.where(zl == 0, jnp.where(zh == 3, 0, 1), jnp.where(zh == 0, 3, 2))
    passes = (
        jnp.where(zl == 0, jnp.where(zh >= 2, 1, 0), jnp.where((zh + 1) % 4 <= 1, 1, 0)) == 1,
        jnp.where(zl == 0, jnp.where((zh + 1) % 4 <= 1, 1, 0), jnp.where(zh <= 1, 1, 0)) == 1,
    )

    def relay(c):
        for half in range(2):

            @pl.when(passes[half])
            def _():
                whole = passed.at[c, half]
                remote(whole, whole, sent_r.at[c, half], came_r.at[c, half], (row, col)).wait_recv()
                for k in (0, 1, 3, 2):
                    remote(
                        passed.at[c, half, k], x.at[c, part(slot(from_zh, k), 8), :],
                        sent_r.at[c, half], came_b.at[c],
                        at(y, (from_zh + 2) % 4, (core + half) % 2, col),
                    ).start()

    def early_z():
        for j in (2, 1, 3, 0):
            for k in range(4):
                to_y, to_zh = (y + k) % 4, (zh + j) % 4
                source = vec.at[pl.ds(LAST * 8, 8), part(to_y * 4 + to_zh, 2 * piece)]
                target = early.at[to_y, (zh % 2) * 2 + zl]
                device = at(y, to_zh, core, far_x * 2 + upper)
                if j % 2:
                    remote(source, target, sent_e, came_e, device).start()
                else:

                    @pl.when(local)
                    def _():
                        if j == 0:
                            pltpu.make_async_copy(source, target, came_e).start()
                        else:
                            remote(
                                source, passed_early.at[k // 2, k % 2], sent_e, came_pe.at[k // 2],
                                at(y, (zh + way(k // 2)) % 4, core, far_x * 2 + upper),
                            ).start()

                    @pl.when(jnp.logical_not(local))
                    def _():
                        remote(source, target, sent_e, came_e, device).start()

    def early_relay():
        for half in range(2):

            @pl.when(passes[half])
            def _():
                whole = passed_early.at[half]
                remote(whole, whole, sent_pe.at[half], came_pe.at[half], (row, col)).wait_recv()
                for i in range(2):
                    remote(
                        passed_early.at[half, i], early.at[(y + half * 2 + i) % 4, (from_zh % 2) * 2 + zl],
                        sent_pe.at[half], came_e, at(y, (from_zh + 2) % 4, core, col),
                    ).start()

    def early_y():
        remote(early, early, sent_e, came_e, (row, col)).wait_recv()
        return {
            k: send(
                early.at[(y + k) % 4], risen.at[k - 1], sent_u.at[k - 1], came_u.at[k - 1], in_y(k)
            )
            for k in (1, 3, 2)
        }

    def early_x(before):
        for k in (0, 1, 3, 2):
            if k:
                before[k].wait_recv()
            origin = (y - k) % 4
            for q in range(4):
                for flip in range(2):
                    to_core = (core + flip) % 2
                    lanes = part(to_core, piece)
                    source = risen.at[k - 1, q, :, lanes] if k else early.at[y, q, :, lanes]
                    place = (q // 2 * 2 + core) * 8 + far_x * 2 + q % 2
                    target = x.at[LAST, part(place, 8), :]
                    there = remote(
                        source, target, sent_b.at[LAST], came_b.at[LAST], at(y, zh, to_core, origin * 2 + zl)
                    )
                    if flip:
                        there.start()
                    else:

                        @pl.when(origin == far_x)
                        def _():
                            pltpu.make_async_copy(source, target, came_b.at[LAST]).start()

                        @pl.when(origin != far_x)
                        def _():
                            there.start()

    early_z()
    begin(1)
    begin(2)
    turn(0)
    from_x = [send(refl, mine, sent_v.at[k], came_v.at[k], in_x(k)) for k in (1, 3, 2)]
    early_relay()
    second(0)
    beside.wait_recv()
    from_z = [send(others, others, sent_v.at[3 + k], came_v.at[3 + k], in_x(k)) for k in (1, 3, 2)]
    turn(1)
    relay(0)
    turn(2)
    rising = early_y()
    for copy in from_x + from_z:
        copy.wait_recv()
    keep.wait()
    for k in range(count):
        vh[k], vl[k] = halves(panels[k])

    line = col % count
    for d in range(1, 4):
        other = (line + d) % count
        low, high = jnp.minimum(line, other), jnp.maximum(line, other)
        gp[d - 1] = dot3((vh[low], vl[low]), (vh[high], vl[high]), NT)
    lot = block // 8
    step_1 = []
    for o in range(1, 8):
        to_y, to_core = (y + o // 2) % 4, (core + o) % 2
        step_1.append(
            send(
                gp.at[:, part(to_core * 4 + to_y, lot), :], g1.at[o - 1],
                sent_g.at[0, o], came_g.at[0, o], at(to_y, zh, to_core, col),
            )
        )
    def g_sum():
        for copy in step_1:
            copy.wait_recv()
        total = gp[:, part(core * 4 + y, lot), :]
        for o in range(7):
            total = total + g1[o]
        gs[...] = total
        return [send(gs, g2.at[k - 1], sent_g.at[1, k], came_g.at[1, k], in_z(k)) for k in (1, 3, 2)]

    def g_col(before):
        for copy in before:
            copy.wait_recv()
        gc[col] = gs[...] + g2[0] + (g2[1] + g2[2])
        return [
            send(gc.at[col], gc.at[col], sent_g.at[2, k], came_g.at[2, k], (row, (col + k) % 8))
            for k in range(1, 8)
        ]

    def g_y(before):
        for copy in before:
            copy.wait_recv()
        lines = part(core * 4 + y, lot)
        gall[:, :, lines, :] = gc[pl.ds(0, count)]
        return [
            send(
                gc.at[pl.ds(0, count)], gall.at[:, :, lines, :],
                sent_g.at[3, k], came_g.at[3, k], in_y(k),
            )
            for k in (1, 3, 2)
        ]

    def g_core(before):
        for copy in before:
            copy.wait_recv()
        lines = part(core, block // 2)
        return send(gall.at[:, :, lines, :], gall.at[:, :, lines, :], sent_g.at[4, 0], came_g.at[4, 0], twin)

    def whole_factor(before):
        before.wait_recv()

        def cross(a, b):
            return gall[a, b - a - 1] if b - a <= 3 else gall[b, count - (b - a) - 1]

        last = count * block
        th[...] = jnp.zeros_like(th)
        tl[...] = jnp.zeros_like(tl)
        for k in range(count - 1, -1, -1):
            inner = halves(factors[k])
            lines, start = pl.ds(k * block, block), (k + 1) * block
            th[lines, lines], tl[lines, lines] = inner
            if start < last:
                rest = pl.ds(start, last - start)
                crossed = jnp.concatenate([cross(k, b) for b in range(k + 1, count)], axis=1)
                met = dot3(halves(crossed), (th[rest, rest], tl[rest, rest]), NN)
                th[lines, rest], tl[lines, rest] = halves(-dot3(inner, halves(met), NN))

    def project(c):
        whole = x.at[c]
        remote(whole, whole, sent_b.at[c], came_b.at[c], (row, col)).wait_recv()
        xh[...], xl[...] = halves(x[c])

        def two(p, carry):
            pair = pl.ds(p * 2, 2)
            right = [ref[pair].reshape(2 * block, piece) for ref in (vh, vl)]
            both = dot3((xh[...], xl[...]), right, NT)
            proj[c, p * 2] = both[:, :block]
            proj[c, p * 2 + 1] = both[:, block:]
            return carry

        lax.fori_loop(0, count // 2, two, 0)
        half = proj.shape[2] // 2
        return [
            send(proj.at[c, :, part(1 - core, half), :], r1.at[c], sent_p.at[c, 0], came_p.at[c, 0], twin)
        ]

    def sum_core(c, before):
        before[0].wait_recv()
        half = proj.shape[2] // 2
        r1[c] = r1[c] + proj[c, :, part(core, half), :]
        return [
            send(
                r1.at[c, :, part((y + k) % 4, half // 4), :], r2.at[c, k - 1],
                sent_p.at[c, k], came_p.at[c, k], in_y(k),
            )
            for k in (1, 3, 2)
        ]

    def sum_y(c, before):
        for copy in before:
            copy.wait_recv()
        s2[c] = r1[c, :, part(y, 32), :] + r2[c, 0] + (r2[c, 1] + r2[c, 2])
        return [
            send(
                s2.at[c, :, part((zh + k) % 4, 8), :], r3.at[c, k - 1],
                sent_p.at[c, 3 + k], came_p.at[c, 3 + k], in_z(k),
            )
            for k in (1, 3, 2)
        ]

    def update(c, before):
        for copy in before:
            copy.wait_recv()
        total = s2[c, :, part(zh, 8), :] + r3[c, 0] + (r3[c, 1] + r3[c, 2])
        flat = jnp.concatenate([total[k] for k in range(count)], axis=1)
        high, low = halves(flat)
        stack = jnp.concatenate([high.astype(F32), low.astype(F32)], axis=0).astype(BF16)
        values = []
        for p in range(0, count, 2):
            lines, rest = pl.ds(p * block, 2 * block), pl.ds(p * block, (count - p) * block)
            both = lax.dot_general(stack[:, p * block :], th[lines, rest], NT, preferred_element_type=F32)
            less = lax.dot_general(high[:, p * block :], tl[lines, rest], NT, preferred_element_type=F32)
            values.append(both[:8] + (both[8:] + less))
        value = jnp.concatenate(values, axis=1)
        lines = part((core * 4 + y) * 4 + zh, 8)
        for k in range(count):
            upd[c, k, lines, :] = value[:, k * block : (k + 1) * block]
        ref = upd.at[c, :, lines, :]
        return [send(ref, ref, sent_p.at[c, 6 + k], came_p.at[c, 6 + k], in_z(k)) for k in (1, 3, 2)]

    def all_z(c, before):
        for copy in before:
            copy.wait_recv()
        ref = upd.at[c, :, part(core * 4 + y, 32), :]
        return [send(ref, ref, sent_p.at[c, 9 + k], came_p.at[c, 9 + k], in_y(k)) for k in (1, 3, 2)]

    def all_y(c, before):
        for copy in before:
            copy.wait_recv()
        ref = upd.at[c, :, part(core, 128), :]
        return [send(ref, ref, sent_p.at[c, 13], came_p.at[c, 13], twin)]

    def finish(c, before):
        before[0].wait_recv()
        flat = jnp.concatenate([upd[c, k] for k in range(count)], axis=1)
        uh[...], ul[...] = halves(flat)
        wide = 256

        def tile(t, carry):
            lanes = part(t, wide)
            right = [ref[:, :, lanes].reshape(count * block, wide) for ref in (vh, vl)]
            moved = x[c, :, lanes] - dot3((uh[...], ul[...]), right, NN)
            out[:, c, :, lanes] = moved.reshape(32, 8, wide)
            return carry

        lax.fori_loop(0, piece // wide, tile, 0)

    at_0 = project(0)
    g = g_sum()
    second(1, (0, 1))
    at_0 = sum_core(0, at_0)
    g = g_col(g)
    at_0 = sum_y(0, at_0)
    second(1, (3, 2), False)
    early_x(rising)
    second(2)
    relay(1)
    at_3 = project(3)
    g = g_y(g)
    at_3 = sum_core(3, at_3)
    g = g_core(g)
    at_1 = project(1)
    relay(2)
    at_3 = sum_y(3, at_3)
    whole_factor(g)
    at_1 = sum_core(1, at_1)
    at_0 = update(0, at_0)
    at_1 = sum_y(1, at_1)
    at_2 = project(2)
    at_2 = sum_core(2, at_2)
    at_3 = update(3, at_3)
    at_1 = update(1, at_1)
    at_0 = all_z(0, at_0)
    at_2 = sum_y(2, at_2)
    at_3 = all_z(3, at_3)
    at_1 = all_z(1, at_1)
    at_0 = all_y(0, at_0)
    at_2 = update(2, at_2)
    at_3 = all_y(3, at_3)
    finish(0, at_0)
    at_2 = all_z(2, at_2)
    at_1 = all_y(1, at_1)
    finish(3, at_3)
    at_2 = all_y(2, at_2)
    finish(1, at_1)
    finish(2, at_2)

    for c in range(LAST):
        three = turned.at[c, pl.ds(0, 3)]
        remote(three, three, sent_t.at[c], came_t.at[c, 0], (row, col)).wait_send()

        @pl.when(local)
        def _():
            some = x.at[c, pl.ds(0, x.shape[1] - 32), :]
            remote(some, some, sent_b.at[c], came_b.at[c], (row, col)).wait_send()

        @pl.when(jnp.logical_not(local))
        def _():
            remote(x.at[c], x.at[c], sent_b.at[c], came_b.at[c], (row, col)).wait_send()

        for half in range(2):

            @pl.when(passes[half])
            def _():
                whole = passed.at[c, half]
                remote(whole, whole, sent_r.at[c, half], came_r.at[c, half], (row, col)).wait_send()

    sent = x.at[LAST, pl.ds(0, x.shape[1] - 32), :]
    remote(sent, sent, sent_b.at[LAST], came_b.at[LAST], (row, col)).wait_send()

    @pl.when(local)
    def _():
        some = early.at[pl.ds(0, 3)]
        remote(some, some, sent_e, came_e, (row, col)).wait_send()

    @pl.when(jnp.logical_not(local))
    def _():
        remote(early, early, sent_e, came_e, (row, col)).wait_send()

    for half in range(2):

        @pl.when(passes[half])
        def _():
            whole = passed_early.at[half]
            remote(whole, whole, sent_pe.at[half], came_pe.at[half], (row, col)).wait_send()

    for copy in pending:
        copy.wait_send()


def on_device(vectors, reflectors, factors):
    count, block = factors.shape[:2]
    rows, length = vectors.shape
    piece = length // 32
    lot = rows * 32 // CHUNKS
    vmem = pltpu.VMEM
    dma = pltpu.SemaphoreType.DMA
    out = pl.pallas_call(
        kernel,
        out_shape=vmem((32, CHUNKS, rows // CHUNKS, piece), F32),
        in_specs=[
            pl.BlockSpec(memory_space=pl.ANY),
            pl.BlockSpec(memory_space=pl.ANY),
            pl.BlockSpec(memory_space=vmem),
        ],
        out_specs=pl.BlockSpec(memory_space=vmem),
        scratch_shapes=[
            vmem((CHUNKS, lot, piece), F32),
            vmem((LAST, 3, 8, 8 * piece), F32),
            vmem((LAST, 4, 8, 8 * piece), F32),
            vmem((LAST, 2, 4, 8, piece), F32),
            vmem((4, 4, 8, 2 * piece), F32),
            vmem((3, 4, 8, 2 * piece), F32),
            vmem((2, 2, 8, 2 * piece), F32),
            vmem((count, block, piece), F32),
            vmem((count, block, piece), BF16),
            vmem((count, block, piece), BF16),
            vmem((lot, piece), BF16),
            vmem((lot, piece), BF16),
            vmem((lot, count * block), BF16),
            vmem((lot, count * block), BF16),
            vmem((CHUNKS, count, lot, block), F32),
            vmem((CHUNKS, count, lot // 2, block), F32),
            vmem((CHUNKS, 3, count, lot // 8, block), F32),
            vmem((CHUNKS, count, lot // 8, block), F32),
            vmem((CHUNKS, 3, count, lot // 32, block), F32),
            vmem((CHUNKS, count, lot, block), F32),
            vmem((3, block, block), F32),
            vmem((7, 3, block // 8, block), F32),
            vmem((3, block // 8, block), F32),
            vmem((3, 3, block // 8, block), F32),
            vmem((8, 3, block // 8, block), F32),
            vmem((count, 3, block, block), F32),
            vmem((count * block, count * block), BF16),
            vmem((count * block, count * block), BF16),
            dma((CHUNKS, 3)),
            dma((CHUNKS, 3)),
            dma((CHUNKS,)),
            dma((CHUNKS, 4)),
            dma((CHUNKS, 2)),
            dma((CHUNKS, 2)),
            dma((CHUNKS,)),
            dma((CHUNKS,)),
            dma,
            dma,
            dma((2,)),
            dma((2,)),
            dma((3,)),
            dma((3,)),
            dma((7,)),
            dma((7,)),
            dma,
            dma((5, 8)),
            dma((5, 8)),
            dma((CHUNKS, 14)),
            dma((CHUNKS, 14)),
        ],
        compiler_params=pltpu.CompilerParams(
            collective_id=1, has_side_effects=True, vmem_limit_bytes=52 * 2**20
        ),
    )(vectors, reflectors, factors)
    return out.reshape(rows * 32, piece)


def solution(mesh):
    placed = (P(("row", "col"), None), P(None, "col", "row"), P())
    return jax.shard_map(
        on_device, mesh=mesh, in_specs=placed, out_specs=P("col", "row"), check_vma=False
    )
```
